32 devices in a mesh: gx: 4 (over z), gy: 8 (over y, x, core).
Axes of the slice: x: 2, y: 2, z: 4, core: 2. Of those that a mesh axis runs over, the one named last changes fastest.
Arguments:
- features: bfloat16 [40960, 2048], P(('gx', 'gy')), may hold values from -6 to 6
- counts: int32 [32], P(('gx', 'gy')), may hold values from 128 to 1280, as said below
- ref_mean: float32 [2048], replicated, may hold values from -6 to 6
- ref_root: float32 [2048, 2048], P('gx', 'gy'), as said below
Outputs:
- mean: float32 [2048], replicated
- root: float32 [2048, 2048], P('gx', 'gy')
- distance: float32 [], replicated
The draws below stay inside these ranges and needn't reach their ends.
Inputs may be any that keep to these rules, and one draw needn't show every extreme that they name: Entry b counts the valid rows of shard b, which come first in it; a multiple of 128; some shard is full in every draw. `ref_root`: symmetric and positive definite.
All inputs are finite; a program needn't handle non-finite values.
Results may differ from the reference program's by a relative error of at most 0.0015.
The reference program's roundings to bfloat16 on the way count: a program that leaves them out, or rounds other values in their place, can miss the bound.
Values may be sent and summed in bfloat16 or wider, within the bound.
A program may use at most 128 MiB of HBM per device.

```python
import jax
import jax.numpy as jnp
from jax import lax

D = 2048
ROWS_DEV = 1280
ITERS = 4
SHARDS = 32


def draw_features(key, part):
    values = jax.random.normal(jax.random.fold_in(key, 27), (SHARDS, ROWS_DEV, D), jnp.float32)
    values = jnp.clip(values, -6.0, 6.0)
    return values.reshape(SHARDS * ROWS_DEV, D).astype(jnp.bfloat16)


def draw_counts(key, part):
    blocks = jax.random.randint(key, (SHARDS,), 1, ROWS_DEV // 128 + 1)
    chosen = jax.random.randint(jax.random.fold_in(key, 7), (), 0, SHARDS)
    blocks = jnp.where(jnp.arange(SHARDS) == chosen, ROWS_DEV // 128, blocks)
    return (blocks * 128).astype(jnp.int32)


def draw_ref_root(key, part):
    noise = jax.random.normal(jax.random.fold_in(key, 11), (D, D), jnp.float32)
    offdiag = (noise + noise.T) * (0.3 / jnp.sqrt(2.0 * D))
    order = jax.random.permutation(jax.random.fold_in(key, 17), D)
    picked = (order < 8).astype(jnp.float32)
    signs = (jax.random.randint(jax.random.fold_in(key, 19), (D,), 0, 2) * 2 - 1).astype(jnp.float32)
    direction = picked * signs / jnp.sqrt(jnp.float32(8.0))
    diag_values = jax.random.uniform(jax.random.fold_in(key, 13), (D,), jnp.float32, 1.0, 2.0)
    strength = jnp.float32(32.0)
    spike = strength * direction[:, None] * direction[None, :]
    return (offdiag + jnp.diag(diag_values) + spike).astype(jnp.float32)


def centred(stream_key, extent, spread, reach, kind=jnp.bfloat16):
    drawn = spread * jax.random.normal(stream_key, extent, jnp.float32)
    return jnp.clip(drawn, min=-reach, max=reach).astype(kind)


def setup_inputs(seed: int = 0) -> dict:
    seeds = jax.random.split(jax.random.key(seed), 5)
    features = draw_features(jax.random.fold_in(seeds[4], 71), 0)
    counts = draw_counts(jax.random.fold_in(seeds[4], 71), 0)
    ref_mean = centred(seeds[2], (D,), 1.0, 6.0, jnp.float32)
    ref_root = draw_ref_root(jax.random.fold_in(seeds[4], 71), 0)
    return {"features": features, "counts": counts, "ref_mean": ref_mean, "ref_root": ref_root}


def rounded(matrix):
    return matrix.astype(jnp.bfloat16)

def product(left, right):
    return jnp.dot(rounded(left), rounded(right), preferred_element_type=jnp.float32)

def reference(features, counts, ref_mean, ref_root):
    blocks = features.reshape(SHARDS, ROWS_DEV, D)

    def accumulate(running, inputs):
        block, count = inputs
        keep = (jnp.arange(ROWS_DEV, dtype=jnp.int32) < count)[:, None]
        whole = block.astype(jnp.float32)
        masked = jnp.where(keep, whole, jnp.float32(0.0))
        added = jnp.dot(masked.T, whole, precision=lax.Precision.HIGHEST)
        return (running + added, lax.optimization_barrier(jnp.sum(masked, axis=0)))
    gram, column_sums = lax.scan(accumulate, jnp.zeros((D, D), jnp.float32), (blocks, counts))
    total = lax.optimization_barrier(jnp.sum(column_sums, axis=0))
    count = jnp.sum(counts).astype(jnp.float32)
    mean = total / count
    cov = (gram - count * mean[:, None] * mean[None, :]) / (count - 1.0)
    half = product(cov, ref_root)
    prod = product(ref_root, half)
    scale = jnp.sqrt(jnp.sum(prod * prod) + 1.0)
    identity = jnp.eye(D, dtype=jnp.float32)
    current = prod / scale
    partner = identity
    for step in range(ITERS):
        middle = 1.5 * identity - 0.5 * product(partner, current)
        current, partner = (product(current, middle), product(middle, partner))
    root = jnp.sqrt(scale) * current
    distance = (jnp.sum((mean - ref_mean) ** 2) + jnp.trace(cov) + jnp.sum(ref_root * ref_root) - 2.0 * jnp.sqrt(scale) * jnp.trace(current)) / 64.0
    return (mean, root, distance)
```

```python
import functools

import jax
import jax.numpy as jnp
from jax import lax
from jax.experimental import pallas as pl
from jax.experimental.pallas import tpu as pltpu
from jax.sharding import PartitionSpec as P

MESH = pl.DeviceIdType.MESH
F32 = jnp.float32
BF16 = jnp.bfloat16


def dot(a, b):
    return jnp.dot(a, b, preferred_element_type=F32)


def chain_kernel(nx, ny, bm, bn, cov_ref, root_ref, part_ref, tile_ref, sums_ref,
                 a, b, c, e, f, prod, ycol, wcol, acc, norm, slots, load_sem, send, recv,
                 norm_send, norm_recv, sum_send, sum_recv):
    width = a.shape[0]
    half = width // 2
    chunks = width // bm
    tr, tc = width // nx, width // ny
    mx, my = lax.axis_index("gx"), lax.axis_index("gy")
    mine = lax.rem(my, 2)
    partner = (mx, my + 1 - 2 * mine)
    col0 = pl.multiple_of(mine * half, half)
    cols = pl.ds(col0, half)

    def load(k, src, dst, s):
        i, j = k // ny, lax.rem(k, ny)
        return pltpu.make_async_copy(
            src.at[pl.ds(pl.multiple_of(k * tr, tr), tr), :],
            dst.at[pl.ds(pl.multiple_of(i * tr, tr), tr), pl.ds(pl.multiple_of(j * tc, tc), tc)],
            load_sem.at[s, k])

    @pl.loop(0, nx * ny)
    def _(k):
        load(k, cov_ref, c, 0).start()
        load(k, root_ref, b, 1).start()

    barrier = pltpu.get_barrier_semaphore()

    def other(d):
        q = d + 1
        return lax.rem(mx + q // ny, nx), lax.rem(my + lax.rem(q, ny), ny)

    def source(d):
        q = d + 1
        return lax.rem(mx + nx - q // ny, nx), lax.rem(my + ny - lax.rem(q, ny), ny)

    @pl.loop(0, nx * ny - 1)
    def _(d):
        pl.semaphore_signal(barrier, inc=1, device_id=other(d), device_id_type=MESH)
    pl.semaphore_wait(barrier, nx * ny - 1)

    @pl.loop(0, nx * ny)
    def _(k):
        load(k, cov_ref, c, 0).wait()
        load(k, root_ref, b, 1).wait()

    def rows_of(k):
        return pl.ds(pl.multiple_of(k * bm, bm), bm)

    def copy(buf, s, k):
        return pltpu.make_async_remote_copy(
            src_ref=buf.at[rows_of(k), cols], dst_ref=buf.at[rows_of(k), cols],
            send_sem=send.at[s, k], recv_sem=recv.at[s, k],
            device_id=partner, device_id_type=MESH)

    def arrived(buf, s, k):
        copy(buf, s, k).wait()

    def blocks(k, left, right, put):
        @pl.loop(0, half // bn)
        def _(n):
            cs = pl.ds(pl.multiple_of(col0 + n * bn, bn), bn)
            put(k, n, cs, dot(left[rows_of(k), :], right[:, cs]))

    def diag(r0, c0, shape):
        r = lax.broadcasted_iota(jnp.int32, shape, 0) + r0
        q = lax.broadcasted_iota(jnp.int32, shape, 1) + c0
        return r == q

    def middle(t, r0, c0):
        return jnp.where(diag(r0, c0, t.shape), 1.5, 0.0) - 0.5 * t

    @pl.loop(0, chunks)
    def _(k):
        def put(k, n, cs, v):
            e[rows_of(k), cs] = v.astype(BF16)
        blocks(k, c, b, put)

    acc[...] = jnp.zeros_like(acc)

    @pl.loop(0, chunks)
    def _(k):
        def put(k, n, cs, v):
            prod[rows_of(k), pl.ds(pl.multiple_of(n * bn, bn), bn)] = v
            acc[...] += jnp.sum((v * v).reshape(bm // 8, 8, bn), axis=0)
        blocks(k, b, e, put)
    norm[0] = jnp.full((8, 128), jnp.sum(acc[...]), F32)
    swap = pltpu.make_async_remote_copy(
        src_ref=norm.at[0], dst_ref=norm.at[1], send_sem=norm_send, recv_sem=norm_recv,
        device_id=partner, device_id_type=MESH)
    swap.start()
    swap.wait()
    scale = jnp.sqrt(norm[0] + norm[1] + 1.0)
    scale_one = scale[0:1, 0:1]

    @pl.loop(0, chunks)
    def _(k):
        @pl.loop(0, half // bn)
        def _(n):
            cs = pl.ds(pl.multiple_of(col0 + n * bn, bn), bn)
            y = (prod[rows_of(k), pl.ds(pl.multiple_of(n * bn, bn), bn)] / scale_one).astype(BF16)
            a[rows_of(k), cs] = y
            b[rows_of(k), cs] = middle(y.astype(F32), k * bm, col0 + n * bn).astype(BF16)
        copy(a, 0, k).start()
        copy(b, 1, k).start()

    def stage(left, right, out, wait, s, mid=False):
        @pl.loop(0, chunks)
        def _(k):
            for buf, w in wait:
                arrived(buf, w, k)

            def put(k, n, cs, v):
                if mid:
                    v = middle(v, k * bm, col0 + n * bn)
                out[rows_of(k), cs] = v.astype(BF16)
            blocks(k, left, right, put)
            copy(out, s, k).start()

    stage(a, b, e, [(a, 0)], 2)
    stage(b, e, c, [(b, 1)], 3, True)
    stage(c, b, f, [(c, 3)], 4)
    stage(e, c, a, [(e, 2)], 5)
    stage(f, a, b, [(f, 4)], 6, True)
    stage(b, f, e, [(b, 6)], 7)

    @pl.loop(0, chunks)
    def _(k):
        arrived(a, 5, k)

    my_rows = pl.ds(pl.multiple_of(mx * tr, tr), tr)
    my_cols = pl.ds(pl.multiple_of(my * tc, tc), tc)

    @pl.loop(0, width // bn)
    def _(n):
        cs = pl.ds(pl.multiple_of(n * bn, bn), bn)
        c[pl.ds(0, tr), cs] = dot(a[my_rows, :], b[:, cs]).astype(BF16)

    @pl.loop(0, chunks)
    def _(k):
        ycol[rows_of(k), :] = dot(a[rows_of(k), :], b[:, my_cols]).astype(BF16)

    @pl.loop(0, chunks)
    def _(k):
        arrived(e, 7, k)
        t = dot(e[rows_of(k), :], ycol[...])
        wcol[rows_of(k), :] = middle(t, k * bm, my * tc).astype(BF16)

    last = dot(c[pl.ds(0, tr), :], wcol[...])
    tile_ref[...] = last
    trace = jnp.sum(jnp.where(diag(mx * tr, my * tc, last.shape), last, 0.0))
    line = lax.broadcasted_iota(jnp.int32, (8, 128), 0)
    me = mx * ny + my
    slots[me] = part_ref[...] + jnp.where(line == 2, trace, 0.0)

    def share(dev, slot):
        return pltpu.make_async_remote_copy(
            src_ref=slots.at[slot], dst_ref=slots.at[slot],
            send_sem=sum_send.at[slot], recv_sem=sum_recv.at[slot],
            device_id=dev, device_id_type=MESH)

    def share_to(d):
        ox, oy = other(d)
        return pltpu.make_async_remote_copy(
            src_ref=slots.at[me], dst_ref=slots.at[me],
            send_sem=sum_send.at[ox * ny + oy], recv_sem=sum_recv.at[me],
            device_id=(ox, oy), device_id_type=MESH)

    @pl.loop(0, nx * ny - 1)
    def _(d):
        share_to(d).start()

    @pl.loop(0, nx * ny - 1)
    def _(d):
        sx, sy = source(d)
        share((sx, sy), sx * ny + sy).wait_recv()

    @pl.loop(0, nx * ny - 1)
    def _(d):
        share_to(d).wait_send()
    sums_ref[...] = jnp.sum(slots[...], axis=0) + jnp.where(line == 3, scale, 0.0)


def chain(nx, ny, cov_tiles, root_tiles, part):
    width = nx * (cov_tiles.shape[0] // (nx * ny))
    half = width // 2
    tr, tc = width // nx, width // ny
    bm, bn = 512, 512
    chunks = width // bm
    n = nx * ny
    return pl.pallas_call(
        functools.partial(chain_kernel, nx, ny, bm, bn),
        name="chain",
        out_shape=(jax.ShapeDtypeStruct((tr, tc), F32), jax.ShapeDtypeStruct((8, 128), F32)),
        in_specs=[pl.BlockSpec(memory_space=pl.ANY)] * 2 + [pl.BlockSpec(memory_space=pltpu.VMEM)],
        out_specs=(pl.BlockSpec(memory_space=pltpu.VMEM), pl.BlockSpec(memory_space=pltpu.VMEM)),
        scratch_shapes=[pltpu.VMEM((width, width), BF16)] * 5 + [
            pltpu.VMEM((width, half), F32),
            pltpu.VMEM((width, tc), BF16),
            pltpu.VMEM((width, tc), BF16),
            pltpu.VMEM((8, bn), F32),
            pltpu.VMEM((2, 8, 128), F32),
            pltpu.VMEM((n, 8, 128), F32),
            pltpu.SemaphoreType.DMA((2, n)),
            pltpu.SemaphoreType.DMA((8, chunks)),
            pltpu.SemaphoreType.DMA((8, chunks)),
            pltpu.SemaphoreType.DMA,
            pltpu.SemaphoreType.DMA,
            pltpu.SemaphoreType.DMA((n,)),
            pltpu.SemaphoreType.DMA((n,)),
        ],
        compiler_params=pltpu.CompilerParams(
            collective_id=0, has_side_effects=True, vmem_limit_bytes=62 * 2**20),
    )(cov_tiles, root_tiles, part)


def shards(nx, ny, features, counts, ref_mean, ref_root):
    width = features.shape[1]
    slots = features.shape[0]
    tile_rows = width // nx
    tile_cols = width // ny
    both = ("gx", "gy")
    root_tiles = lax.all_gather(ref_root.astype(BF16), both, axis=0, tiled=True)
    keep = (jnp.arange(slots, dtype=jnp.int32) < counts[0])[:, None]
    masked = jnp.where(keep, features, jnp.zeros_like(features))
    partial_gram = lax.dot_general(
        masked, features, (((0,), (0,)), ((), ())), preferred_element_type=F32
    )
    column_total = jnp.sum(masked.astype(F32), axis=0)
    local_count = counts[0].astype(F32)
    total, count = lax.psum((column_total, local_count), both)
    column_block = lax.psum_scatter(partial_gram, "gy", scatter_dimension=1, tiled=True)
    gram_tile = lax.psum_scatter(column_block, "gx", scatter_dimension=0, tiled=True)
    mean = total / count
    row_start = lax.axis_index("gx") * tile_rows
    col_start = lax.axis_index("gy") * tile_cols
    mean_rows = lax.dynamic_slice_in_dim(mean, row_start, tile_rows, 0)
    mean_cols = lax.dynamic_slice_in_dim(mean, col_start, tile_cols, 0)
    cov_tile = (gram_tile - count * mean_rows[:, None] * mean_cols[None, :]) / (count - 1.0)
    row_ids = jnp.arange(tile_rows, dtype=jnp.int32) + row_start
    col_ids = jnp.arange(tile_cols, dtype=jnp.int32) + col_start
    on_diag = row_ids[:, None] == col_ids[None, :]
    cov_tiles = lax.all_gather(cov_tile.astype(BF16), both, axis=0, tiled=True)
    line = lax.broadcasted_iota(jnp.int32, (8, 128), 0)
    part = jnp.where(
        line == 0, jnp.sum(jnp.where(on_diag, cov_tile, 0.0)),
        jnp.where(line == 1, jnp.sum(ref_root * ref_root), 0.0))
    tile, sums = chain(nx, ny, cov_tiles, root_tiles, part)
    scale = sums[3, 0]
    root = jnp.sqrt(scale) * tile
    distance = (
        jnp.sum((mean - ref_mean) ** 2) + sums[0, 0] + sums[1, 0]
        - 2.0 * jnp.sqrt(scale) * sums[2, 0]
    ) / 64.0
    return (mean, root, distance)


def solution(mesh):
    return jax.shard_map(
        functools.partial(shards, mesh.shape["gx"], mesh.shape["gy"]),
        mesh=mesh,
        in_specs=(P(("gx", "gy"), None), P(("gx", "gy")), P(), P("gx", "gy")),
        out_specs=(P(), P("gx", "gy"), P()),
        check_vma=False,
    )
```
